1024 devices in a mesh: outer: 16 (over y, core), inner: 64 (over z, x).
Axes of the slice: x: 4, y: 8, z: 16, core: 2. Of those that a mesh axis runs over, the one named last changes fastest.
Arguments:
- queries: bfloat16 [131072, 16, 128], P(('outer', 'inner')), may hold values from -160 to 160
- key_vectors: bfloat16 [131072, 128], P(('outer', 'inner')), may hold values from -6 to 6
- value_vectors: bfloat16 [131072, 128], P(('outer', 'inner')), may hold values from -6 to 6
- doc_lengths: int32 [128], replicated, may hold values from 1 to 1921, 131072 in all
Outputs:
- attended: bfloat16 [131072, 16, 128], P(('outer', 'inner'))
The draws below stay inside these ranges and needn't reach their ends.
All inputs are finite; a program needn't handle non-finite values.
Results may differ from the reference program's by a relative error of at most 0.0037.
Values may be sent and summed in bfloat16 or wider, within the bound.
A program may use at most 32 MiB of HBM per device.

```python
import math
import jax
import jax.numpy as jnp
import numpy as np
from jax import lax

HEADS = 16
HDIM = 128
TOK_DEV = 128
REACH = 16
TOKENS = 131072
DOCMAX = 1921
DOCS = 128


def paired_draw(key):
    base_keys = jax.random.truncated_normal(jax.random.fold_in(key, 3), -6.0, 6.0, (TOKENS, HDIM), jnp.float32)
    base_queries = jax.random.truncated_normal(jax.random.fold_in(key, 4), -6.0, 6.0, (TOKENS, HEADS, HDIM), jnp.float32)
    return (base_queries, base_keys)


def draw_queries(key, part):
    return paired_draw(key)[0].astype(jnp.bfloat16)


def draw_key_vectors(key, part):
    return paired_draw(key)[1].astype(jnp.bfloat16)


def steps_of(stream_key, dims, pieces, smallest, largest):
    gain, own = 1.0, jax.random.fold_in(stream_key, 6)
    for dim, parts in pieces:
        steps = jnp.exp(jax.random.uniform(jax.random.fold_in(own, dim), (parts,), jnp.float32, smallest / len(pieces), largest / len(pieces)))
        gain = gain * jnp.repeat(steps, dims[dim] // parts).reshape([-1 if axis == dim else 1 for axis in range(len(dims))])
    return gain


def profile(number_of, total, limit, slope):
    portions = [(1 << 20) // math.isqrt(grade ** slope) + 1 for grade in range(2, number_of + 1)]
    surplus, counts = total - limit - (number_of - 1), [1] * (number_of - 1)
    while surplus > 0:
        candidates = [i for i in range(number_of - 1) if counts[i] < limit]
        whole, remaining = sum([portions[i] for i in candidates]), surplus
        for i in candidates:
            extra = min(limit - counts[i], max(1, remaining * portions[i] // whole), surplus)
            counts[i] = counts[i] + extra
            surplus = surplus - extra
    return np.array([limit] + counts)


def uneven(key, count, total, limit, slope):
    if count == 2:
        one = jax.random.randint(key, (), max(1, total - limit), min(limit, total - 1) + 1)
        return jnp.stack([one, total - one])
    sizes = jnp.asarray(profile(count, total, limit, slope), jnp.int32)
    twos = (count - 1) // 2
    giver, receiver = sizes[1:1 + 2 * twos:2], sizes[2:2 + 2 * twos:2]
    room = jnp.minimum(giver - 1, limit - receiver)
    moved = jax.random.randint(jax.random.fold_in(key, 1), (twos,), 0, 1 << 20) % (room + 1)
    sizes = sizes.at[1:1 + 2 * twos:2].set(giver - moved).at[2:2 + 2 * twos:2].set(receiver + moved)
    return sizes[jax.random.permutation(jax.random.fold_in(key, 2), count)]


def bell_draw(own_key, dims, scale, limit, split=(), held_as=jnp.bfloat16):
    factor_of = steps_of(own_key, dims, split, -0.22, 0.18) if split else 1.0
    values = jax.random.normal(own_key, dims, jnp.float32) * scale * factor_of
    return jnp.minimum(jnp.maximum(values, -limit), limit).astype(held_as)


def setup_inputs(seed: int = 0) -> dict:
    key_list = jax.random.split(jax.random.key(seed), 5)
    return {
        "queries": draw_queries(jax.random.fold_in(key_list[4], 71), 0),
        "key_vectors": draw_key_vectors(jax.random.fold_in(key_list[4], 71), 0),
        "value_vectors": bell_draw(key_list[2], (TOKENS, HDIM), 1.0, 6.0, ((0, 1024),)),
        "doc_lengths": uneven(key_list[3], DOCS, TOKENS, DOCMAX, 2).astype(jnp.int32),
    }


def segment_ids(positions, starts):
    inside = (starts[None, :] <= positions[:, None]).astype(jnp.int32)
    return jnp.sum(inside, axis=1).astype(jnp.int32) - 1


def update(running, query_rows, key_rows, value_rows, query_seg, query_pos, key_seg, key_pos):
    row_max, row_sum, accumulated = running
    scale_factor = query_rows.shape[-1] ** -0.5
    scores = jnp.einsum("thd,kd->thk", query_rows.astype(jnp.float32), key_rows.astype(jnp.float32)) * scale_factor
    allowed = (query_seg[:, None] == key_seg[None, :]) & (key_pos[None, :] <= query_pos[:, None])
    scores = jnp.where(allowed[:, None, :], scores, -1e30)
    new_max = jnp.maximum(row_max, jnp.max(scores, axis=-1))
    rescale = jnp.exp(row_max - new_max)
    weights = jnp.exp(scores - new_max[..., None])
    row_sum = rescale * row_sum + jnp.sum(weights, axis=-1)
    rounded = weights.astype(jnp.bfloat16)
    product = jnp.einsum("thk,kd->thd", rounded.astype(jnp.float32), value_rows.astype(jnp.float32))
    accumulated = rescale[..., None] * accumulated + product
    return (new_max, row_sum, accumulated)


def reference(queries, key_vectors, value_vectors, doc_lengths):
    starts = (jnp.cumsum(doc_lengths) - doc_lengths).astype(jnp.int32)
    blocks = TOKENS // TOK_DEV
    padding = jnp.zeros(((REACH - 1) * TOK_DEV, HDIM), key_vectors.dtype)
    key_padded = jnp.concatenate([padding, key_vectors], axis=0)
    value_padded = jnp.concatenate([padding, value_vectors], axis=0)
    offsets = jnp.arange(TOK_DEV, dtype=jnp.int32)

    def query_block(block):
        query_rows = lax.dynamic_slice_in_dim(queries, (block * TOK_DEV).astype(jnp.int32), TOK_DEV, 0)
        query_pos = block * TOK_DEV + offsets
        query_seg = segment_ids(query_pos, starts)
        running = (jnp.full((TOK_DEV, HEADS), -1e30, jnp.float32),
                   jnp.zeros((TOK_DEV, HEADS), jnp.float32),
                   jnp.zeros((TOK_DEV, HEADS, HDIM), jnp.float32))
        for distance in range(REACH - 1, -1, -1):
            begin = ((block - distance + REACH - 1) * TOK_DEV).astype(jnp.int32)
            key_rows = lax.dynamic_slice_in_dim(key_padded, begin, TOK_DEV, 0)
            value_rows = lax.dynamic_slice_in_dim(value_padded, begin, TOK_DEV, 0)
            key_pos = (block - distance) * TOK_DEV + offsets
            key_seg = segment_ids(key_pos, starts)
            running = update(running, query_rows, key_rows, value_rows, query_seg, query_pos, key_seg, key_pos)
        return (running[2] / running[1][..., None]).astype(jnp.bfloat16)

    result = lax.map(query_block, jnp.arange(blocks, dtype=jnp.int32))
    return result.reshape(TOKENS, HEADS, HDIM)
```

```python
import jax
import jax.numpy as jnp
from jax import lax
from jax.experimental import pallas as pl
from jax.experimental.pallas import tpu as pltpu
from jax.sharding import PartitionSpec as P

MESH = pl.DeviceIdType.MESH
BLK = 128
NX = 4
NZ = 16
ROWS = 5
NEG = -1e30
TILE = 256
UNROLL = 2


def kernel(
    q_ref, k_ref, v_ref, dl_ref, o_ref,
    hold, qa, ka, acc, m_sc, l_sc, out_sc, dl_sc,
    ssem, rsem, lsem, osem,
):
    inner = lax.axis_size("inner")
    total = inner * lax.axis_size("outer")
    b = lax.axis_index("outer") * inner + lax.axis_index("inner")
    x = lax.rem(b, NX)
    r = b // NX
    z = lax.rem(r, NZ)

    def dev(dz, dx):
        x2 = lax.rem(x + dx + NX, NX)
        t = lax.rem(b - x + x2 + NX * dz + total, total)
        return (t // inner, lax.rem(t, inner))

    def slot(k, c):
        return (ROWS - 1 - k) * NX + lax.rem(x + c + NX, NX)

    sends = []

    def copy_of(h, k, c, dz, dx):
        src = slot(k, c)
        dst = src - NX * dz
        i = len(sends)
        return pltpu.make_async_remote_copy(
            src_ref=hold.at[src, h],
            dst_ref=hold.at[dst, h],
            send_sem=ssem.at[i],
            recv_sem=rsem.at[dst, h],
            device_id=dev(dz, dx),
            device_id_type=MESH,
        )

    def send(cond, h, k, c, dz, dx):
        cp = copy_of(h, k, c, dz, dx)
        sends.append((cond, cp))
        pl.when(cond)(cp.start)

    def recv(cond, h, k, c):
        sl = slot(k, c)

        def wait():
            pltpu.make_async_copy(hold.at[sl, h], hold.at[sl, h], rsem.at[sl, h]).wait()

        pl.when(cond)(wait)

    def mid(k):
        return (k >= 1) & (k <= 3)

    def has(k):
        return r >= k

    last = total // NX - 1

    def next_has(dz):
        return r + dz <= last

    bar = pltpu.get_barrier_semaphore()

    def say(dz, dx):
        pl.semaphore_signal(bar, inc=1, device_id=dev(dz, dx), device_id_type=MESH)

    say(0, 1)
    say(0, -1)
    pl.when(has(1))(lambda: say(-1, 0))
    for d in (2, 3, 4):
        pl.when((z == 0) & has(d))(lambda d=d: say(-d, 0))

    mine = slot(0, 0)
    kcp = pltpu.make_async_copy(k_ref, hold.at[mine, 0], lsem.at[0])
    vcp = pltpu.make_async_copy(v_ref, hold.at[mine, 1], lsem.at[1])
    qcp = pltpu.make_async_copy(q_ref, qa.at[:, pl.ds(0, 128)], lsem.at[2])
    dcp = pltpu.make_async_copy(dl_ref, dl_sc, lsem.at[3])
    kcp.start()
    vcp.start()
    dcp.start()
    qcp.start()

    direct = [(z == NZ - d) & next_has(d) for d in (2, 3, 4)]
    peers = 2 + next_has(1).astype(jnp.int32)
    for cond in direct:
        peers = peers + cond.astype(jnp.int32)
    pl.semaphore_wait(bar, peers)

    kcp.wait()
    vcp.wait()

    def level_one(k, h):
        right = mid(k) | ((k == 0) & (x < 3)) | ((k == 4) & (x == 3))
        left = mid(k) | ((k == 0) & (x == 0)) | ((k == 4) & (x > 0))
        send(right & has(k), h, k, 0, 0, 1)
        send(left & has(k), h, k, 0, 0, -1)

    def level_two(k):
        inside = (x == 1) | (x == 2)
        from_left = mid(k) | ((k == 0) & (x > 0)) | ((k == 4) & (x == 0))
        from_right = mid(k) | ((k == 0) & (x == 3)) | ((k == 4) & (x < 3))
        for h in (0, 1):
            recv(from_left & has(k), h, k, -1)
            recv(from_right & has(k), h, k, 1)
            both_right = (k == 0) & inside
            both_left = (k == 4) & inside
            if h == 0:
                send((mid(k) | both_right) & has(k), h, k, -1, 0, 1)
                send(both_left & has(k), h, k, 1, 0, -1)
            else:
                send((mid(k) | both_left) & has(k), h, k, 1, 0, -1)
                send(both_right & has(k), h, k, -1, 0, 1)

    def opposite(k):
        cond = mid(k) | ((k == 0) & (x >= 2)) | ((k == 4) & (x <= 1))
        for h in (0, 1):
            recv(cond & has(k), h, k, 2)

    for h in (0, 1):
        send(next_has(1), h, 0, 0, 1, 0)
        for d, cond in zip((2, 3, 4), direct):
            send(cond & ((d < 4) | (x > 0)), h, 0, 0, d, 0)
    for h in (0, 1):
        level_one(0, h)

    for k in range(1, ROWS):

        def clear(k=k):
            rows = pl.ds((ROWS - 1 - k) * NX, NX)
            hold[rows] = jnp.zeros((NX,) + hold.shape[1:], hold.dtype)

        pl.when(jnp.logical_not(has(k)))(clear)
    dcp.wait()
    lengths = dl_sc[...].astype(jnp.float32)
    ii = lax.broadcasted_iota(jnp.int32, (BLK, BLK), 0)
    jj = lax.broadcasted_iota(jnp.int32, (BLK, BLK), 1)
    starts = jnp.sum(jnp.where(jj < ii, lengths, 0.0), axis=1, keepdims=True)
    pos_q = (b * BLK + jj).astype(jnp.float32)
    low = jnp.max(jnp.where(starts <= pos_q, starts, 0.0), axis=0, keepdims=True)
    high = pos_q[0:1]
    base = (b - 15) * BLK

    def one_bias(i, carry):
        pos_k = (base + i * BLK + ii).astype(jnp.float32)
        ok = (pos_k >= low) & (pos_k <= high)
        ka[pl.ds(pl.multiple_of(i * BLK, BLK), BLK), pl.ds(128, 128)] = jnp.where(
            ok, 0.0, NEG
        ).astype(jnp.bfloat16)
        return carry

    lax.fori_loop(0, 16, one_bias, 0)

    def one_hot(i, carry):
        row = i * BLK + ii
        qa[pl.ds(pl.multiple_of(i * BLK, BLK), BLK), pl.ds(128, 128)] = jnp.where(
            row // 16 == jj, 1.0, 0.0
        ).astype(jnp.bfloat16)
        return carry

    lax.fori_loop(0, 16, one_hot, 0)

    early = jnp.minimum(z, 4)
    order = [0 * z]
    for s in range(1, 5):
        order.append(jnp.where(s <= early, s, early + 5 - s))
    for s in range(1, 5):
        k = order[s]
        exists = has(k) & ((k < 4) | (x > 0))
        for h in (0, 1):
            recv(exists, h, k, 0)
            onward = mid(k) & has(k) & next_has(1) & (z != NZ - 1)
            send(onward & ((k < 3) | (x > 0)), h, k, 0, 1, 0)
            level_one(k, h)
        level_two(order[s - 1])

    qcp.wait()
    scale = 128 ** (-0.5) * 1.4426950408889634
    outs = []

    def run(s):
        j = jnp.where(s < early, 3 - s, s - early)
        first = x + 1 + NX * j
        kbase = pl.multiple_of(j * 512, 512)
        for i in range(NX):
            ka[pl.ds(pl.multiple_of(kbase + i * BLK, BLK), BLK), pl.ds(0, 128)] = hold[first + i, 0]
        keys = ka[pl.ds(kbase, 512), :]
        values = hold[pl.ds(first, NX), 1].reshape(512, 128)

        def tile(t):
            rows = pl.ds(pl.multiple_of(t * TILE, TILE), TILE)
            sc = lax.dot_general(
                qa[rows, :], keys, (((1,), (1,)), ((), ())), preferred_element_type=jnp.float32
            )
            top = jnp.max(sc, axis=1, keepdims=True)
            if s > 0:
                m_old = m_sc[rows, 0:1]
                top = jnp.maximum(top, m_old)
            w = jnp.exp2((sc - top) * scale)
            total_w = jnp.sum(w, axis=1, keepdims=True)
            part = jnp.dot(w.astype(jnp.bfloat16), values, preferred_element_type=jnp.float32)
            if s > 0:
                alpha = jnp.exp2((m_old - top) * scale)
                total_w = total_w + alpha * l_sc[rows, 0:1]
                part = part + alpha * acc[rows, :]
            if s < 3:
                m_sc[rows, :] = jnp.broadcast_to(top, (TILE, 128))
                l_sc[rows, :] = jnp.broadcast_to(total_w, (TILE, 128))
                acc[rows, :] = part
            else:
                out_sc[rows, :] = (part / total_w).astype(jnp.bfloat16)

        def body(i, carry):
            for u in range(UNROLL):
                tile(i * UNROLL + u)
            if s == 3:
                rows = pl.ds(pl.multiple_of(i * TILE * UNROLL, TILE * UNROLL), TILE * UNROLL)
                pltpu.make_async_copy(out_sc.at[rows], o_ref.at[rows], osem.at[i]).start()
            return carry

        n = 2048 // (TILE * UNROLL)
        lax.fori_loop(0, n, body, 0)
        if s == 3:
            for i in range(n):
                rows = pl.ds(i * TILE * UNROLL, TILE * UNROLL)
                pltpu.make_async_copy(out_sc.at[rows], o_ref.at[rows], osem.at[i]).wait()

    opposite(order[0])
    opposite(order[1])
    opposite(order[2])
    run(0)
    opposite(order[3])
    run(1)
    level_two(order[4])
    opposite(order[4])
    run(2)
    run(3)
    for cond, cp in sends:
        pl.when(cond)(cp.wait_send)


def body(queries, key_vectors, value_vectors, doc_lengths):
    tok, heads, dim = queries.shape
    rows = tok * heads
    any_spec = pl.BlockSpec(memory_space=pl.ANY)
    out = pl.pallas_call(
        kernel,
        out_shape=jax.ShapeDtypeStruct((rows, dim), jnp.bfloat16),
        in_specs=[any_spec] * 4,
        out_specs=any_spec,
        scratch_shapes=[
            pltpu.VMEM((ROWS * NX, 2, BLK, dim), jnp.bfloat16),
            pltpu.VMEM((rows, 256), jnp.bfloat16),
            pltpu.VMEM((16 * BLK, 256), jnp.bfloat16),
            pltpu.VMEM((rows, 128), jnp.float32),
            pltpu.VMEM((rows, 128), jnp.float32),
            pltpu.VMEM((rows, 128), jnp.float32),
            pltpu.VMEM((rows, 128), jnp.bfloat16),
            pltpu.VMEM((1, 128), jnp.int32),
            pltpu.SemaphoreType.DMA((72,)),
            pltpu.SemaphoreType.DMA((ROWS * NX, 2)),
            pltpu.SemaphoreType.DMA((4,)),
            pltpu.SemaphoreType.DMA((16,)),
        ],
        compiler_params=pltpu.CompilerParams(collective_id=0, has_side_effects=True),
    )(queries.reshape(rows, dim), key_vectors, value_vectors, doc_lengths.reshape(1, -1))
    return out.reshape(tok, heads, dim)


def solution(mesh):
    in_specs = (
        P(("outer", "inner"), None, None),
        P(("outer", "inner"), None),
        P(("outer", "inner"), None),
        P(),
    )
    out_specs = P(("outer", "inner"), None, None)
    return jax.shard_map(body, mesh=mesh, in_specs=in_specs, out_specs=out_specs, check_vma=False)
```

```python
import jax
import jax.numpy as jnp
from jax import lax
from jax.experimental import pallas as pl
from jax.experimental.pallas import tpu as pltpu
from jax.sharding import PartitionSpec as P

MESH = pl.DeviceIdType.MESH
BLK = 128
NX = 4
NZ = 16
ROWS = 5
NEG = -1e30
TILE = 512
NSEND = 46


def kernel(
    q_ref, k_ref, v_ref, dl_ref, o_ref,
    hold, qa, ka, acc, m_sc, l_sc, out_sc, dl_sc,
    ssem, rsem, lsem, osem,
):
    inner = lax.axis_size("inner")
    total = inner * lax.axis_size("outer")
    b = lax.axis_index("outer") * inner + lax.axis_index("inner")
    x = lax.rem(b, NX)
    r = b // NX
    z = lax.rem(r, NZ)

    def dev(dz, dx):
        x2 = lax.rem(x + dx + NX, NX)
        t = lax.rem(b - x + x2 + NX * dz + total, total)
        return (t // inner, lax.rem(t, inner))

    def slot(k, c):
        return (ROWS - 1 - k) * NX + lax.rem(x + c + NX, NX)

    sends = {}

    def copy_of(i, h, k, c, dz, dx):
        src = slot(k, c)
        dst = src - NX * dz
        return pltpu.make_async_remote_copy(
            src_ref=hold.at[src, h],
            dst_ref=hold.at[dst, h],
            send_sem=ssem.at[i],
            recv_sem=rsem.at[dst, h],
            device_id=dev(dz, dx),
            device_id_type=MESH,
        )

    def send(cond, key, h, k, c, dz, dx):
        key = key + (h,)
        i, before = sends.get(key, (len(sends), []))
        cp = copy_of(i, h, k, c, dz, dx)
        sends[key] = (i, before + [(cond, cp)])
        pl.when(cond)(cp.start)

    def recv(cond, h, k, c):
        sl = slot(k, c)

        def wait():
            pltpu.make_async_copy(hold.at[sl, h], hold.at[sl, h], rsem.at[sl, h]).wait()

        pl.when(cond)(wait)

    def mid(k):
        return (k >= 1) & (k <= 3)

    def has(k):
        return r >= k

    last = total // NX - 1

    def next_has(dz):
        return r + dz <= last

    early = jnp.minimum(z, 4)

    def row_at(i):
        return jnp.where((i <= early) | (early >= 2) | (i == 0), i, early + 5 - i)

    order = [row_at(i) for i in range(ROWS)]

    bar = pltpu.get_barrier_semaphore()

    def say(dz, dx):
        pl.semaphore_signal(bar, inc=1, device_id=dev(dz, dx), device_id_type=MESH)

    say(0, 1)
    say(0, -1)
    pl.when(has(1))(lambda: say(-1, 0))
    for d in (2, 3, 4):
        pl.when((z == 0) & has(d))(lambda d=d: say(-d, 0))
    pl.when((z == 3) & has(4))(lambda: say(-4, 0))
    pl.when((z == 2) & has(3))(lambda: say(-3, 0))

    mine = slot(0, 0)
    kcp = pltpu.make_async_copy(k_ref, hold.at[mine, 0], lsem.at[0])
    vcp = pltpu.make_async_copy(v_ref, hold.at[mine, 1], lsem.at[1])
    qcp = pltpu.make_async_copy(q_ref, qa.at[:, pl.ds(0, 128)], lsem.at[2])
    dcp = pltpu.make_async_copy(dl_ref, dl_sc, lsem.at[3])
    kcp.start()
    vcp.start()
    dcp.start()
    qcp.start()

    last_row = z == NZ - 1
    reach = jnp.where(last_row, 3, NZ - z)
    over = (z >= NZ - 4) & (r + reach <= last) & (last_row | (z > NZ - 4) | (x > 0))
    peers = 2 + next_has(1).astype(jnp.int32)
    peers = peers + ((z >= NZ - 4) & (r + reach <= last)).astype(jnp.int32)
    peers = peers + (last_row & next_has(4)).astype(jnp.int32)
    pl.semaphore_wait(bar, peers)

    kcp.wait()
    vcp.wait()

    def level_one(i, h):
        k = order[i]
        right = mid(k) | ((k == 0) & (x < 3)) | ((k == 4) & (x == 3))
        left = mid(k) | ((k == 0) & (x == 0)) | ((k == 4) & (x > 0))
        send(right & has(k), ("right", i), h, k, 0, 0, 1)
        send(left & has(k), ("left", i), h, k, 0, 0, -1)

    def level_two(i, when):
        k = order[i]
        inside = (x == 1) | (x == 2)
        from_left = when & (mid(k) | ((k == 0) & (x > 0)) | ((k == 4) & (x == 0)))
        from_right = when & (mid(k) | ((k == 0) & (x == 3)) | ((k == 4) & (x < 3)))
        onward = when & has(k) & (mid(k) | inside)
        for h in (0, 1):
            recv(from_left & has(k), h, k, -1)
            recv(from_right & has(k), h, k, 1)
            leftward = (k == 4) | ((k > 0) & (h == 1))
            step = jnp.where(leftward, -1, 1)
            send(onward, ("two", i), h, k, -step, 0, step)

    def opposite(i, when):
        k = order[i]
        cond = when & (mid(k) | ((k == 0) & (x >= 2)) | ((k == 4) & (x <= 1)))
        for h in (0, 1):
            recv(cond & has(k), h, k, 2)

    for h in (0, 1):
        send(next_has(1), ("own",), h, 0, 0, 1, 0)
    for h in (0, 1):
        send(over, ("over",), h, 0, 0, reach, 0)
        send(last_row & next_has(4) & (x > 0), ("far",), h, 0, 0, 4, 0)
    for h in (0, 1):
        level_one(0, h)

    def clear(i, carry):
        k, c = ROWS - 1 - i // NX, lax.rem(i, NX)
        unused = (r < k) | ((k == 0) & (c > x)) | ((k == 4) & ((c < x) | (x + c == 0)))

        def zero():
            hold[i] = jnp.zeros(hold.shape[1:], hold.dtype)

        pl.when(unused)(zero)
        return carry

    lax.fori_loop(0, ROWS * NX, clear, 0)
    dcp.wait()
    lengths = dl_sc[...].astype(jnp.float32)
    ii = lax.broadcasted_iota(jnp.int32, (BLK, BLK), 0)
    jj = lax.broadcasted_iota(jnp.int32, (BLK, BLK), 1)
    starts = jnp.sum(jnp.where(jj < ii, lengths, 0.0), axis=1, keepdims=True)
    pos_q = (b * BLK + jj).astype(jnp.float32)
    low = jnp.max(jnp.where(starts <= pos_q, starts, 0.0), axis=0, keepdims=True)
    high = pos_q[0:1]
    base = (r - (ROWS - 1)) * (NX * BLK)

    def one_bias(i, carry):
        pos_k = (base + i * BLK + ii).astype(jnp.float32)
        ok = (pos_k >= low) & (pos_k <= high)
        ka[pl.ds(pl.multiple_of(i * BLK, BLK), BLK), pl.ds(128, 128)] = jnp.where(
            ok, 0.0, NEG
        ).astype(jnp.bfloat16)
        return carry

    lax.fori_loop(0, ROWS * NX, one_bias, 0)

    def one_hot(i, carry):
        row = i * BLK + ii
        qa[pl.ds(pl.multiple_of(i * BLK, BLK), BLK), pl.ds(128, 128)] = jnp.where(
            row // 16 == jj, 1.0, 0.0
        ).astype(jnp.bfloat16)
        return carry

    lax.fori_loop(0, 16, one_hot, 0)
    m_sc[...] = jnp.full_like(m_sc, NEG)
    l_sc[...] = jnp.zeros_like(l_sc)
    acc[...] = jnp.zeros_like(acc)

    scale = 128 ** (-0.5) * 1.4426950408889634

    def pairs(op, parts):
        while len(parts) > 1:
            parts = [op(parts[i], parts[i + 1]) for i in range(0, len(parts), 2)]
        return parts[0]

    def run(k, last=False):
        first = (ROWS - 1 - k) * NX
        kbase = pl.multiple_of(first * BLK, NX * BLK)
        for i in range(NX):
            ka[pl.ds(pl.multiple_of(kbase + i * BLK, BLK), BLK), pl.ds(0, 128)] = hold[first + i, 0]
        keys = ka[pl.ds(kbase, NX * BLK), :]
        values = hold[pl.ds(first, NX), 1].reshape(NX * BLK, 128)
        for t in range(2048 // TILE):
            rows = pl.ds(t * TILE, TILE)
            sc = lax.dot_general(
                qa[rows, :], keys, (((1,), (1,)), ((), ())), preferred_element_type=jnp.float32
            )
            cols = [sc[:, g * 128 : (g + 1) * 128] for g in range(4)]
            top = jnp.max(pairs(jnp.maximum, cols), axis=1, keepdims=True)
            m_old = m_sc[rows, :]
            top = jnp.maximum(jnp.broadcast_to(top, (TILE, 128)), m_old)
            ws = [jnp.exp2((c - top) * scale) for c in cols]
            w = jnp.concatenate([c.astype(jnp.bfloat16) for c in ws], axis=1)
            part = jnp.dot(w, values, preferred_element_type=jnp.float32)
            alpha = jnp.exp2((m_old - top) * scale)
            total_w = pairs(jnp.add, ws) + alpha * l_sc[rows, :]
            part = part + alpha * acc[rows, :]
            if last:
                norm = jnp.sum(total_w, axis=1, keepdims=True)
                out_sc[rows, :] = (part / norm).astype(jnp.bfloat16)
                pltpu.make_async_copy(out_sc.at[rows], o_ref.at[rows], osem.at[t]).start()
            else:
                m_sc[rows, :] = top
                l_sc[rows, :] = total_w
                acc[rows, :] = part

    def runs(lo, hi):
        def one(i, carry):
            run(row_at(i))
            return carry

        lax.fori_loop(lo, hi, one, 0)

    for s in range(1, 5):
        k = order[s]
        turn = s == early + 1
        level_two(s - 1, turn)
        for i in range(s):
            opposite(i, turn)
        if s == 1:
            qcp.wait()
        runs(0, jnp.where(turn, s, 0))
        if s == 4:
            level_two(3, early == 2)
            opposite(3, early == 2)
            runs(3, jnp.where(early == 2, 4, 3))
        exists = has(k) & ((k < 4) | (x > 0))
        for h in (0, 1):
            recv(exists, h, k, 0)
            onward = mid(k) & has(k) & next_has(1) & jnp.logical_not(last_row)
            skip = ((k == 2) & (z == 1)) | ((k == 3) & ((x == 0) | (z == 2)))
            send(onward & jnp.logical_not(skip), ("on", s), h, k, 0, 1, 0)
            level_one(s, h)
        level_two(s - 1, (s <= early) | ((s > early + 1) & (s < 4)))
    level_two(3, early < 2)
    opposite(1, early == 0)
    runs(1, jnp.where(early == 0, 2, 1))
    level_two(4, early >= 0)
    for i in range(3):
        opposite(i, (early == 4) | ((i == 2) & (early < 2)))
    lo = jnp.where(early == 4, 0, jnp.where(early < 2, 2, 4))
    runs(lo, jnp.where(lo == 4, 4, 3))
    opposite(3, (early == 4) | (early < 2))
    runs(jnp.where(lo == 4, 4, 3), 4)
    opposite(4, early >= 0)
    run(order[4], last=True)
    for t in range(2048 // TILE):
        rows = pl.ds(t * TILE, TILE)
        pltpu.make_async_copy(out_sc.at[rows], o_ref.at[rows], osem.at[t]).wait()
    assert len(sends) <= NSEND
    for i, copies in sends.values():
        cond = copies[0][0]
        for other, cp in copies[1:]:
            cond = cond | other
        pl.when(cond)(copies[0][1].wait_send)


def body(queries, key_vectors, value_vectors, doc_lengths):
    tok, heads, dim = queries.shape
    rows = tok * heads
    any_spec = pl.BlockSpec(memory_space=pl.ANY)
    out = pl.pallas_call(
        kernel,
        out_shape=jax.ShapeDtypeStruct((rows, dim), jnp.bfloat16),
        in_specs=[any_spec] * 4,
        out_specs=any_spec,
        scratch_shapes=[
            pltpu.VMEM((ROWS * NX, 2, BLK, dim), jnp.bfloat16),
            pltpu.VMEM((rows, 256), jnp.bfloat16),
            pltpu.VMEM((ROWS * NX * BLK, 256), jnp.bfloat16),
            pltpu.VMEM((rows, 128), jnp.float32),
            pltpu.VMEM((rows, 128), jnp.float32),
            pltpu.VMEM((rows, 128), jnp.float32),
            pltpu.VMEM((rows, 128), jnp.bfloat16),
            pltpu.VMEM((1, 128), jnp.int32),
            pltpu.SemaphoreType.DMA((NSEND,)),
            pltpu.SemaphoreType.DMA((ROWS * NX, 2)),
            pltpu.SemaphoreType.DMA((4,)),
            pltpu.SemaphoreType.DMA((4,)),
        ],
        compiler_params=pltpu.CompilerParams(collective_id=0, has_side_effects=True),
    )(queries.reshape(rows, dim), key_vectors, value_vectors, doc_lengths.reshape(1, -1))
    return out.reshape(tok, heads, dim)


def solution(mesh):
    in_specs = (
        P(("outer", "inner"), None, None),
        P(("outer", "inner"), None),
        P(("outer", "inner"), None),
        P(),
    )
    out_specs = P(("outer", "inner"), None, None)
    return jax.shard_map(body, mesh=mesh, in_specs=in_specs, out_specs=out_specs, check_vma=False)
```

```python
import jax
import jax.numpy as jnp
from jax import lax
from jax.experimental import pallas as pl
from jax.experimental.pallas import tpu as pltpu
from jax.sharding import PartitionSpec as P

MESH = pl.DeviceIdType.MESH
BLK = 128
NX = 4
NZ = 16
ROWS = 5
NEG = -1e30
TILE = 256
NSEND = 42


def kernel(
    q_ref, k_ref, v_ref, dl_ref, o_ref,
    hold, qa, ka, acc, m_sc, l_sc, out_sc, dl_sc,
    ssem, rsem, lsem, osem,
):
    inner = lax.axis_size("inner")
    total = inner * lax.axis_size("outer")
    b = lax.axis_index("outer") * inner + lax.axis_index("inner")
    x = lax.rem(b, NX)
    r = b // NX
    z = lax.rem(r, NZ)

    def dev(dz, dx):
        x2 = lax.rem(x + dx + NX, NX)
        t = lax.rem(b - x + x2 + NX * dz + total, total)
        return (t // inner, lax.rem(t, inner))

    def slot(k, c):
        return (ROWS - 1 - k) * NX + lax.rem(x + c + NX, NX)

    sends = {}

    def copy_of(i, h, k, c, dz, dx):
        src = slot(k, c)
        dst = src - NX * dz
        return pltpu.make_async_remote_copy(
            src_ref=hold.at[src, h],
            dst_ref=hold.at[dst, h],
            send_sem=ssem.at[i],
            recv_sem=rsem.at[dst, h],
            device_id=dev(dz, dx),
            device_id_type=MESH,
        )

    def send(cond, key, h, k, c, dz, dx):
        key = key + (h,)
        i, before = sends.get(key, (len(sends), []))
        cp = copy_of(i, h, k, c, dz, dx)
        sends[key] = (i, before + [(cond, cp)])
        pl.when(cond)(cp.start)

    def recv(cond, h, k, c):
        sl = slot(k, c)

        def wait():
            pltpu.make_async_copy(hold.at[sl, h], hold.at[sl, h], rsem.at[sl, h]).wait()

        pl.when(cond)(wait)

    def mid(k):
        return (k >= 1) & (k <= 3)

    def has(k):
        return r >= k

    last = total // NX - 1

    def next_has(dz):
        return r + dz <= last

    early = jnp.minimum(z, 4)

    def row_at(i):
        return jnp.where((i <= early) | (i == 0), i, early + 5 - i)

    order = [row_at(i) for i in range(ROWS)]

    bar = pltpu.get_barrier_semaphore()

    def say(dz, dx):
        pl.semaphore_signal(bar, inc=1, device_id=dev(dz, dx), device_id_type=MESH)

    say(0, 1)
    say(0, -1)
    pl.when(has(1))(lambda: say(-1, 0))
    for d in (2, 3, 4):
        pl.when((z == 0) & has(d))(lambda d=d: say(-d, 0))
    pl.when((z == 3) & has(4))(lambda: say(-4, 0))

    mine = slot(0, 0)
    kcp = pltpu.make_async_copy(k_ref, hold.at[mine, 0], lsem.at[0])
    vcp = pltpu.make_async_copy(v_ref, hold.at[mine, 1], lsem.at[1])
    qcp = pltpu.make_async_copy(q_ref, qa.at[:, pl.ds(0, 128)], lsem.at[2])
    dcp = pltpu.make_async_copy(dl_ref, dl_sc, lsem.at[3])
    kcp.start()
    vcp.start()
    dcp.start()
    qcp.start()

    last_row = z == NZ - 1
    reach = jnp.where(last_row, 4, NZ - z)
    afar = (z >= NZ - 4) & (r + reach <= last)
    over = afar & ((x > 0) | (reach < 4))
    peers = 2 + next_has(1).astype(jnp.int32) + afar.astype(jnp.int32)
    pl.semaphore_wait(bar, peers)

    kcp.wait()
    vcp.wait()

    def level_one(i, h):
        k = order[i]
        right = mid(k) | ((k == 0) & (x < 3)) | ((k == 4) & (x == 3))
        left = mid(k) | ((k == 0) & (x == 0)) | ((k == 4) & (x > 0))
        send(right & has(k), ("right", i), h, k, 0, 0, 1)
        send(left & has(k), ("left", i), h, k, 0, 0, -1)

    def level_two(i, when):
        k = order[i]
        inside = (x == 1) | (x == 2)
        from_left = when & (mid(k) | ((k == 0) & (x > 0)) | ((k == 4) & (x == 0)))
        from_right = when & (mid(k) | ((k == 0) & (x == 3)) | ((k == 4) & (x < 3)))
        onward = when & has(k) & (mid(k) | inside)
        for h in (0, 1):
            recv(from_left & has(k), h, k, -1)
            recv(from_right & has(k), h, k, 1)
            leftward = (k == 4) | ((k > 0) & (h == 1))
            step = jnp.where(leftward, -1, 1)
            send(onward, ("two", i), h, k, -step, 0, step)

    def opposite(i, when):
        k = order[i]
        cond = when & (mid(k) | ((k == 0) & (x >= 2)) | ((k == 4) & (x <= 1)))
        for h in (0, 1):
            recv(cond & has(k), h, k, 2)

    for h in (0, 1):
        send(over & jnp.logical_not(last_row), ("over",), h, 0, 0, reach, 0)
    for h in (0, 1):
        send(next_has(1), ("own",), h, 0, 0, 1, 0)
    for h in (0, 1):
        send(over & last_row, ("over",), h, 0, 0, reach, 0)
    for h in (0, 1):
        level_one(0, h)

    def clear(i, carry):
        k, c = ROWS - 1 - i // NX, lax.rem(i, NX)
        unused = (r < k) | ((k == 0) & (c > x)) | ((k == 4) & ((c < x) | (x + c == 0)))

        def zero():
            hold[i] = jnp.zeros(hold.shape[1:], hold.dtype)

        pl.when(unused)(zero)
        return carry

    lax.fori_loop(0, ROWS * NX, clear, 0)
    dcp.wait()
    lengths = dl_sc[...].astype(jnp.float32)
    ii = lax.broadcasted_iota(jnp.int32, (BLK, BLK), 0)
    jj = lax.broadcasted_iota(jnp.int32, (BLK, BLK), 1)
    starts = jnp.sum(jnp.where(jj < ii, lengths, 0.0), axis=1, keepdims=True)
    pos_q = (b * BLK + jj).astype(jnp.float32)
    low = jnp.max(jnp.where(starts <= pos_q, starts, 0.0), axis=0, keepdims=True)
    high = pos_q[0:1]
    base = (r - (ROWS - 1)) * (NX * BLK)

    def one_bias(i, carry):
        pos_k = (base + i * BLK + ii).astype(jnp.float32)
        ok = (pos_k >= low) & (pos_k <= high)
        row, col = i // NX, lax.rem(i, NX)
        place = jnp.where(row == ROWS - 1, col, NX + col * NX + row)
        ka[pl.ds(pl.multiple_of(place * BLK, BLK), BLK), pl.ds(128, 128)] = jnp.where(
            ok, 0.0, NEG
        ).astype(jnp.bfloat16)
        return carry

    lax.fori_loop(0, ROWS * NX, one_bias, 0)

    def one_hot(i, carry):
        row = i * BLK + ii
        qa[pl.ds(pl.multiple_of(i * BLK, BLK), BLK), pl.ds(128, 128)] = jnp.where(
            row // 16 == jj, 1.0, 0.0
        ).astype(jnp.bfloat16)
        return carry

    lax.fori_loop(0, 16, one_hot, 0)
    m_sc[...] = jnp.full_like(m_sc, NEG)
    l_sc[...] = jnp.zeros_like(l_sc)
    acc[...] = jnp.zeros_like(acc)

    scale = 128 ** (-0.5) * 1.4426950408889634

    def pairs(op, parts):
        while len(parts) > 1:
            parts = [op(parts[i], parts[i + 1]) for i in range(0, len(parts), 2)]
        return parts[0]

    def run(unit, last=False):
        first = jnp.where(unit == 0, (ROWS - 1) * NX, unit - 1)
        step = jnp.where(unit == 0, 1, NX)
        kbase = pl.multiple_of(unit * (NX * BLK), NX * BLK)
        for i in range(NX):
            at = pl.ds(pl.multiple_of(kbase + i * BLK, BLK), BLK)
            ka[at, pl.ds(0, 128)] = hold[first + step * i, 0]
        keys = ka[pl.ds(kbase, NX * BLK), :]
        values = jnp.concatenate([hold[first + step * i, 1] for i in range(NX)], axis=0)

        def score(t):
            return lax.dot_general(
                qa[pl.ds(t * TILE, TILE), :],
                keys,
                (((1,), (1,)), ((), ())),
                preferred_element_type=jnp.float32,
            )

        def weigh(t, sc):
            rows = pl.ds(t * TILE, TILE)
            cols = [sc[:, g * 128 : (g + 1) * 128] for g in range(4)]
            top = jnp.max(pairs(jnp.maximum, cols), axis=1, keepdims=True)
            m_old = m_sc[rows, :]
            top = jnp.maximum(jnp.broadcast_to(top, (TILE, 128)), m_old)
            ws = [jnp.exp2((c - top) * scale) for c in cols]
            alpha = jnp.exp2((m_old - top) * scale)
            m_sc[rows, :] = top
            l_sc[rows, :] = pairs(jnp.add, ws) + alpha * l_sc[rows, :]
            return jnp.concatenate([c.astype(jnp.bfloat16) for c in ws], axis=1), alpha

        def add(t, w, alpha):
            rows = pl.ds(t * TILE, TILE)
            part = jnp.dot(w, values, preferred_element_type=jnp.float32) + alpha * acc[rows, :]
            if last:
                norm = jnp.sum(l_sc[rows, :], axis=1, keepdims=True)
                out_sc[rows, :] = (part / norm).astype(jnp.bfloat16)
                pltpu.make_async_copy(out_sc.at[rows], o_ref.at[rows], osem.at[t]).start()
            else:
                acc[rows, :] = part

        n = 2048 // TILE
        scores, weights = {}, {}
        for u in range(n + 2):
            if u < n:
                scores[u] = score(u)
            if 0 <= u - 1 < n:
                weights[u - 1] = weigh(u - 1, scores.pop(u - 1))
            if 0 <= u - 2:
                add(u - 2, *weights.pop(u - 2))

    def column(c):
        return 1 + lax.rem(x + c + NX, NX)

    level_two(0, early >= 0)
    opposite(0, early >= 0)
    qcp.wait()
    run(0 * z)
    for s in range(1, 5):
        k = order[s]
        if s > 1:
            level_two(s - 1, s == early + 1)
        exists = has(k) & ((k < 4) | (x > 0))
        for h in (0, 1):
            recv(exists, h, k, 0)
            onward = mid(k) & has(k) & next_has(1) & jnp.logical_not(last_row)
            skip = (k == 3) & ((x == 0) | (z == 2))
            send(onward & jnp.logical_not(skip), ("on", s), h, k, 0, 1, 0)
            level_one(s, h)
        if s > 1:
            level_two(s - 1, s <= early)
    for i in (1, 2):
        level_two(i, i > early)
    run(column(0))
    level_two(3, early < 3)
    level_two(4, early >= 0)

    def side(i, carry):
        run(column(2 * i - 1))
        return carry

    lax.fori_loop(0, 2, side, 0)
    for i in range(1, ROWS):
        opposite(i, early >= 0)
    run(column(2), last=True)
    assert len(sends) <= NSEND
    for i, copies in sends.values():
        cond = copies[0][0]
        for other, cp in copies[1:]:
            cond = cond | other
        pl.when(cond)(copies[0][1].wait_send)
    for t in range(2048 // TILE):
        rows = pl.ds(t * TILE, TILE)
        pltpu.make_async_copy(out_sc.at[rows], o_ref.at[rows], osem.at[t]).wait()


def body(queries, key_vectors, value_vectors, doc_lengths):
    tok, heads, dim = queries.shape
    rows = tok * heads
    any_spec = pl.BlockSpec(memory_space=pl.ANY)
    out = pl.pallas_call(
        kernel,
        out_shape=jax.ShapeDtypeStruct((rows, dim), jnp.bfloat16),
        in_specs=[any_spec] * 4,
        out_specs=any_spec,
        scratch_shapes=[
            pltpu.VMEM((ROWS * NX, 2, BLK, dim), jnp.bfloat16),
            pltpu.VMEM((rows, 256), jnp.bfloat16),
            pltpu.VMEM((ROWS * NX * BLK, 256), jnp.bfloat16),
            pltpu.VMEM((rows, 128), jnp.float32),
            pltpu.VMEM((rows, 128), jnp.float32),
            pltpu.VMEM((rows, 128), jnp.float32),
            pltpu.VMEM((rows, 128), jnp.bfloat16),
            pltpu.VMEM((1, 128), jnp.int32),
            pltpu.SemaphoreType.DMA((NSEND,)),
            pltpu.SemaphoreType.DMA((ROWS * NX, 2)),
            pltpu.SemaphoreType.DMA((4,)),
            pltpu.SemaphoreType.DMA((2048 // TILE,)),
        ],
        compiler_params=pltpu.CompilerParams(collective_id=0, has_side_effects=True),
    )(queries.reshape(rows, dim), key_vectors, value_vectors, doc_lengths.reshape(1, -1))
    return out.reshape(tok, heads, dim)


def solution(mesh):
    in_specs = (
        P(("outer", "inner"), None, None),
        P(("outer", "inner"), None),
        P(("outer", "inner"), None),
        P(),
    )
    out_specs = P(("outer", "inner"), None, None)
    return jax.shard_map(body, mesh=mesh, in_specs=in_specs, out_specs=out_specs, check_vma=False)
```

```python
import jax
import jax.numpy as jnp
from jax import lax
from jax.experimental import pallas as pl
from jax.experimental.pallas import tpu as pltpu
from jax.sharding import PartitionSpec as P

MESH = pl.DeviceIdType.MESH
BLK = 128
NX = 4
NZ = 16
ROWS = 5
NEG = -1e30
TILE = 256
NSEND = 42


def kernel(
    q_ref, k_ref, v_ref, dl_ref, o_ref,
    hold, qa, ka, acc, m_sc, l_sc, out_sc, dl_sc,
    ssem, rsem, lsem, osem,
):
    inner = lax.axis_size("inner")
    total = inner * lax.axis_size("outer")
    b = lax.axis_index("outer") * inner + lax.axis_index("inner")
    x = lax.rem(b, NX)
    r = b // NX
    z = lax.rem(r, NZ)

    def dev(dz, dx):
        x2 = lax.rem(x + dx + NX, NX)
        t = lax.rem(b - x + x2 + NX * dz + total, total)
        return (t // inner, lax.rem(t, inner))

    def slot(k, c):
        return (ROWS - 1 - k) * NX + lax.rem(x + c + NX, NX)

    sends = {}

    def copy_of(i, h, k, c, dz, dx):
        src = slot(k, c)
        dst = src - NX * dz
        return pltpu.make_async_remote_copy(
            src_ref=hold.at[src, h],
            dst_ref=hold.at[dst, h],
            send_sem=ssem.at[i],
            recv_sem=rsem.at[dst, h],
            device_id=dev(dz, dx),
            device_id_type=MESH,
        )

    def send(cond, key, h, k, c, dz, dx):
        key = key + (h,)
        i, before = sends.get(key, (len(sends), []))
        cp = copy_of(i, h, k, c, dz, dx)
        sends[key] = (i, before + [(cond, cp)])
        pl.when(cond)(cp.start)

    def recv(cond, h, k, c):
        sl = slot(k, c)

        def wait():
            pltpu.make_async_copy(hold.at[sl, h], hold.at[sl, h], rsem.at[sl, h]).wait()

        pl.when(cond)(wait)

    def mid(k):
        return (k >= 1) & (k <= 3)

    def has(k):
        return r >= k

    last = total // NX - 1

    def next_has(dz):
        return r + dz <= last

    early = jnp.minimum(z, 4)

    def row_at(i):
        return jnp.where((i <= early) | (i == 0), i, early + 5 - i)

    order = [row_at(i) for i in range(ROWS)]

    late = 4 - early

    def slot_of(n):
        m = n - NX * (early + 1)
        turn = sum((m >= late * t).astype(jnp.int32) for t in (1, 2, 3))
        shift = jnp.where(turn == 0, 0, jnp.where(turn == 1, NX - 1, turn - 1))
        late_slot = (m - turn * late) * NX + lax.rem(x + shift, NX)
        early_slot = (ROWS - 1 - n // NX) * NX + lax.rem(n, NX)
        return jnp.where(m < 0, early_slot, late_slot)

    bar = pltpu.get_barrier_semaphore()

    def say(dz, dx):
        pl.semaphore_signal(bar, inc=1, device_id=dev(dz, dx), device_id_type=MESH)

    say(0, 1)
    say(0, -1)
    pl.when(has(1))(lambda: say(-1, 0))
    for d in (2, 3, 4):
        pl.when((z == 0) & has(d))(lambda d=d: say(-d, 0))
    pl.when((z == 3) & has(4))(lambda: say(-4, 0))

    mine = slot(0, 0)
    kcp = pltpu.make_async_copy(k_ref, hold.at[mine, 0], lsem.at[0])
    vcp = pltpu.make_async_copy(v_ref, hold.at[mine, 1], lsem.at[1])
    qcp = pltpu.make_async_copy(q_ref, qa.at[:, pl.ds(0, 128)], lsem.at[2])
    dcp = pltpu.make_async_copy(dl_ref, dl_sc, lsem.at[3])
    kcp.start()
    vcp.start()
    dcp.start()
    qcp.start()

    last_row = z == NZ - 1
    reach = jnp.where(last_row, 4, NZ - z)
    afar = (z >= NZ - 4) & (r + reach <= last)
    over = afar & ((x > 0) | (reach < 4))
    peers = 2 + next_has(1).astype(jnp.int32) + afar.astype(jnp.int32)
    pl.semaphore_wait(bar, peers)

    kcp.wait()
    vcp.wait()

    def level_one(i, h):
        k = order[i]
        right = mid(k) | ((k == 0) & (x < 3)) | ((k == 4) & (x == 3))
        left = mid(k) | ((k == 0) & (x == 0)) | ((k == 4) & (x > 0))
        send(right & has(k), ("right", i), h, k, 0, 0, 1)
        send(left & has(k), ("left", i), h, k, 0, 0, -1)

    def level_two(i, when):
        k = order[i]
        inside = (x == 1) | (x == 2)
        from_left = when & (mid(k) | ((k == 0) & (x > 0)) | ((k == 4) & (x == 0)))
        from_right = when & (mid(k) | ((k == 0) & (x == 3)) | ((k == 4) & (x < 3)))
        onward = when & has(k) & (mid(k) | inside)
        for h in (0, 1):
            recv(from_left & has(k), h, k, -1)
            recv(from_right & has(k), h, k, 1)
            leftward = (k == 4) | ((k > 0) & (h == 1))
            step = jnp.where(leftward, -1, 1)
            send(onward, ("two", i), h, k, -step, 0, step)

    def opposite(i, when):
        k = order[i]
        cond = when & (mid(k) | ((k == 0) & (x >= 2)) | ((k == 4) & (x <= 1)))
        for h in (0, 1):
            recv(cond & has(k), h, k, 2)

    for h in (0, 1):
        send(over & jnp.logical_not(last_row), ("over",), h, 0, 0, reach, 0)
    for h in (0, 1):
        send(next_has(1), ("own",), h, 0, 0, 1, 0)
    for h in (0, 1):
        send(over & last_row, ("over",), h, 0, 0, reach, 0)
    for h in (0, 1):
        level_one(0, h)

    def clear(i, carry):
        k, c = ROWS - 1 - i // NX, lax.rem(i, NX)
        unused = (r < k) | ((k == 0) & (c > x)) | ((k == 4) & ((c < x) | (x + c == 0)))

        def zero():
            hold[i] = jnp.zeros(hold.shape[1:], hold.dtype)

        pl.when(unused)(zero)
        return carry

    lax.fori_loop(0, ROWS * NX, clear, 0)
    dcp.wait()
    lengths = dl_sc[...].astype(jnp.float32)
    ii = lax.broadcasted_iota(jnp.int32, (BLK, BLK), 0)
    jj = lax.broadcasted_iota(jnp.int32, (BLK, BLK), 1)
    starts = jnp.sum(jnp.where(jj < ii, lengths, 0.0), axis=1, keepdims=True)
    pos_q = (b * BLK + jj).astype(jnp.float32)
    low = jnp.max(jnp.where(starts <= pos_q, starts, 0.0), axis=0, keepdims=True)
    high = pos_q[0:1]
    base = (r - (ROWS - 1)) * (NX * BLK)

    def one_bias(i, carry):
        pos_k = (base + slot_of(i) * BLK + ii).astype(jnp.float32)
        ok = (pos_k >= low) & (pos_k <= high)
        ka[pl.ds(pl.multiple_of(i * BLK, BLK), BLK), pl.ds(128, 128)] = jnp.where(
            ok, 0.0, NEG
        ).astype(jnp.bfloat16)
        return carry

    lax.fori_loop(0, ROWS * NX, one_bias, 0)

    def one_hot(i, carry):
        row = i * BLK + ii
        qa[pl.ds(pl.multiple_of(i * BLK, BLK), BLK), pl.ds(128, 128)] = jnp.where(
            row // 16 == jj, 1.0, 0.0
        ).astype(jnp.bfloat16)
        return carry

    lax.fori_loop(0, 16, one_hot, 0)
    m_sc[...] = jnp.full_like(m_sc, NEG)
    l_sc[...] = jnp.zeros_like(l_sc)
    acc[...] = jnp.zeros_like(acc)

    scale = 128 ** (-0.5) * 1.4426950408889634

    def pairs(op, parts):
        while len(parts) > 1:
            parts = [op(parts[i], parts[i + 1]) for i in range(0, len(parts), 2)]
        return parts[0]

    def run(unit, last=False):
        slots = [slot_of(unit * NX + i) for i in range(NX)]
        kbase = pl.multiple_of(unit * (NX * BLK), NX * BLK)
        for i in range(NX):
            at = pl.ds(pl.multiple_of(kbase + i * BLK, BLK), BLK)
            ka[at, pl.ds(0, 128)] = hold[slots[i], 0]
        keys = ka[pl.ds(kbase, NX * BLK), :]
        values = jnp.concatenate([hold[slots[i], 1] for i in range(NX)], axis=0)

        def score(t):
            return lax.dot_general(
                qa[pl.ds(t * TILE, TILE), :],
                keys,
                (((1,), (1,)), ((), ())),
                preferred_element_type=jnp.float32,
            )

        def weigh(t, sc):
            rows = pl.ds(t * TILE, TILE)
            cols = [sc[:, g * 128 : (g + 1) * 128] for g in range(4)]
            top = jnp.max(pairs(jnp.maximum, cols), axis=1, keepdims=True)
            m_old = m_sc[rows, :]
            top = jnp.maximum(jnp.broadcast_to(top, (TILE, 128)), m_old)
            ws = [jnp.exp2((c - top) * scale) for c in cols]
            alpha = jnp.exp2((m_old - top) * scale)
            m_sc[rows, :] = top
            l_sc[rows, :] = pairs(jnp.add, ws) + alpha * l_sc[rows, :]
            return jnp.concatenate([c.astype(jnp.bfloat16) for c in ws], axis=1), alpha

        def add(t, w, alpha):
            rows = pl.ds(t * TILE, TILE)
            part = jnp.dot(w, values, preferred_element_type=jnp.float32) + alpha * acc[rows, :]
            if last:
                norm = jnp.sum(l_sc[rows, :], axis=1, keepdims=True)
                out_sc[rows, :] = (part / norm).astype(jnp.bfloat16)
                pltpu.make_async_copy(out_sc.at[rows], o_ref.at[rows], osem.at[t]).start()
            else:
                acc[rows, :] = part

        n = 2048 // TILE
        scores, weights = {}, {}
        for u in range(n + 2):
            if u < n:
                scores[u] = score(u)
            if 0 <= u - 1 < n:
                weights[u - 1] = weigh(u - 1, scores.pop(u - 1))
            if 0 <= u - 2:
                add(u - 2, *weights.pop(u - 2))

    def runs(lo, hi):
        def one(i, carry):
            run(i)
            return carry

        lax.fori_loop(lo, hi, one, 0)

    level_two(0, early >= 0)
    opposite(0, early >= 0)
    qcp.wait()
    run(0 * z)
    for s in range(1, 5):
        k = order[s]
        if s > 1:
            turn = s == early + 1
            level_two(s - 1, turn)
            for i in range(1, s):
                opposite(i, turn)
            runs(1, jnp.where(turn, s, 1))
        exists = has(k) & ((k < 4) | (x > 0))
        for h in (0, 1):
            recv(exists, h, k, 0)
            onward = mid(k) & has(k) & next_has(1) & jnp.logical_not(last_row)
            skip = (k == 3) & ((x == 0) | (z == 2))
            send(onward & jnp.logical_not(skip), ("on", s), h, k, 0, 1, 0)
            level_one(s, h)
        if s > 1:
            level_two(s - 1, s <= early)
    for i in (1, 2):
        level_two(i, i > early)
    runs(early + 1, jnp.where(early < 2, early + 2, early + 1))
    level_two(3, early < 3)
    level_two(4, early >= 0)
    for i in range(1, ROWS):
        opposite(i, early == 4)
    runs(jnp.where(early == 4, 1, jnp.where(early == 3, 4, jnp.where(early == 0, 2, 3))), 4)
    for i in range(1, ROWS):
        opposite(i, i > early)
    run(4 + 0 * z, last=True)
    assert len(sends) <= NSEND
    for i, copies in sends.values():
        cond = copies[0][0]
        for other, cp in copies[1:]:
            cond = cond | other
        pl.when(cond)(copies[0][1].wait_send)
    for t in range(2048 // TILE):
        rows = pl.ds(t * TILE, TILE)
        pltpu.make_async_copy(out_sc.at[rows], o_ref.at[rows], osem.at[t]).wait()


def body(queries, key_vectors, value_vectors, doc_lengths):
    tok, heads, dim = queries.shape
    rows = tok * heads
    any_spec = pl.BlockSpec(memory_space=pl.ANY)
    out = pl.pallas_call(
        kernel,
        out_shape=jax.ShapeDtypeStruct((rows, dim), jnp.bfloat16),
        in_specs=[any_spec] * 4,
        out_specs=any_spec,
        scratch_shapes=[
            pltpu.VMEM((ROWS * NX, 2, BLK, dim), jnp.bfloat16),
            pltpu.VMEM((rows, 256), jnp.bfloat16),
            pltpu.VMEM((ROWS * NX * BLK, 256), jnp.bfloat16),
            pltpu.VMEM((rows, 128), jnp.float32),
            pltpu.VMEM((rows, 128), jnp.float32),
            pltpu.VMEM((rows, 128), jnp.float32),
            pltpu.VMEM((rows, 128), jnp.bfloat16),
            pltpu.VMEM((1, 128), jnp.int32),
            pltpu.SemaphoreType.DMA((NSEND,)),
            pltpu.SemaphoreType.DMA((ROWS * NX, 2)),
            pltpu.SemaphoreType.DMA((4,)),
            pltpu.SemaphoreType.DMA((2048 // TILE,)),
        ],
        compiler_params=pltpu.CompilerParams(collective_id=0, has_side_effects=True),
    )(queries.reshape(rows, dim), key_vectors, value_vectors, doc_lengths.reshape(1, -1))
    return out.reshape(tok, heads, dim)


def solution(mesh):
    in_specs = (
        P(("outer", "inner"), None, None),
        P(("outer", "inner"), None),
        P(("outer", "inner"), None),
        P(),
    )
    out_specs = P(("outer", "inner"), None, None)
    return jax.shard_map(body, mesh=mesh, in_specs=in_specs, out_specs=out_specs, check_vma=False)
```
